32 devices in a mesh: frag: 2 (over x), dev2: 4 (over z), dev: 4 (over y, core).
Axes of the slice: x: 2, y: 2, z: 4, core: 2. Of those that a mesh axis runs over, the one named last changes fastest.
Arguments:
- ao_ints: bfloat16 [256, 128, 128, 128], P(('frag', 'dev'), 'dev2'), parts along dimension 0
- c_occ: bfloat16 [256, 24], P('frag'), parts along dimension 0
- c_virt: bfloat16 [256, 80], P('frag'), parts along dimension 0
Outputs:
- output: float32 [48, 80, 1920], P('frag', None, ('dev2', 'dev')), parts along dimension 0
There are 2 independent parts. The reference program is written for one: setup_inputs(seed, part) draws one part's arguments, and reference() takes and returns one part's arrays. A program takes and returns all parts, laid end to end along the dimension named above; each array names one.
All inputs are finite; a program needn't handle non-finite values.
Results may differ from the reference program's by a relative error of at most 0.001.
Values are sent between devices in bfloat16 or wider.
A program may use at most 1 GiB of HBM per device.

```python
import jax
import jax.numpy as jnp
from jax import lax

NBF = 128
OCC = 24
VIRT = 80


def setup_inputs(seed: int = 0, part: int = 0) -> dict:
    base_key = jax.random.fold_in(jax.random.key(seed), part)
    key_ao, key_occ, key_virt = jax.random.split(base_key, 3)
    row_keys = jax.random.split(key_ao, NBF)
    ao_ints = lax.map(
        lambda row_key: jax.random.normal(row_key, (NBF, NBF, NBF), jnp.float32).astype(jnp.bfloat16),
        row_keys)
    c_occ = jax.random.normal(key_occ, (NBF, OCC), jnp.float32) * NBF ** -0.5
    c_virt = jax.random.normal(key_virt, (NBF, VIRT), jnp.float32) * NBF ** -0.5
    return {"ao_ints": ao_ints, "c_occ": c_occ.astype(jnp.bfloat16), "c_virt": c_virt.astype(jnp.bfloat16)}


def reference(ao_ints, c_occ, c_virt):
    occ_f32 = c_occ.astype(jnp.float32)
    virt_f32 = c_virt.astype(jnp.float32)

    def half_row(ao_row):
        t_one = jnp.einsum("qrs,rj->qsj", ao_row.astype(jnp.float32), occ_f32).astype(jnp.bfloat16)
        return jnp.einsum("qsj,sb->qjb", t_one.astype(jnp.float32), virt_f32).astype(jnp.bfloat16)

    half_ints = lax.map(half_row, ao_ints).astype(jnp.float32)
    e_part = jnp.einsum("pi,pqjb->iqjb", occ_f32, half_ints)
    mo_ints = jnp.einsum("iqjb,qa->iajb", e_part, virt_f32)
    return mo_ints.reshape(OCC, VIRT, OCC * VIRT)
```

```python
import functools

import jax
import jax.numpy as jnp
from jax import lax
from jax.experimental import pallas as pl
from jax.experimental.pallas import tpu as pltpu
from jax.sharding import PartitionSpec as P

MESH = pl.DeviceIdType.MESH
F32 = jnp.float32
BF16 = jnp.bfloat16
OCC = 24
VIRT = 80
LANES = 120
QSUB = 2
QBLK = 8
STEPS = 32 // QSUB
BLKS = 32 // QBLK
SUBS = QBLK // QSUB
AHEAD = 4


def dot(a, b):
    return jnp.dot(a, b, preferred_element_type=F32)


def dot_nt(a, b):
    return lax.dot_general(a, b, (((1,), (1,)), ((), ())), preferred_element_type=F32)


def iota(shape, dim):
    return lax.broadcasted_iota(jnp.int32, shape, dim)


def select(mask):
    return jnp.where(mask, 1.0, 0.0).astype(BF16)


def kernel(ao_ref, occ_ref, virt_ref, out_ref,
           a_buf, occ_lhs, virt_rhs, kron_own, kron_sib, virt_t,
           h_buf, h_in, e_buf, y_in, e_all,
           a_sem, hs_sem, hr_sem, ys_sem, yr_sem, zs_sem, zr_sem):
    z = lax.axis_index("dev2")
    dev = lax.axis_index("dev")
    y = dev // 2
    core = dev % 2
    sib = y * 2 + (1 - core)
    across = (1 - y) * 2 + core
    half = z // 2
    order = (3 * (1 - half), 2 - half, 1 - z + 4 * half)

    def a_copy(s):
        return pltpu.make_async_copy(
            ao_ref.at[:, pl.ds(s * QSUB, QSUB)], a_buf.at[s], a_sem.at[s])

    def h_copy(s):
        return pltpu.make_async_remote_copy(
            src_ref=h_buf.at[1 - core, pl.ds(s * QSUB, QSUB)],
            dst_ref=h_in.at[pl.ds(s * QSUB, QSUB)],
            send_sem=hs_sem.at[s], recv_sem=hr_sem.at[s],
            device_id={"dev": sib}, device_id_type=MESH)

    def y_copy(blk, zz):
        rows = pl.ds(zz * (OCC * QBLK), OCC * QBLK)
        return pltpu.make_async_remote_copy(
            src_ref=e_buf.at[1 - y, blk, rows], dst_ref=y_in.at[blk, rows],
            send_sem=ys_sem.at[blk, zz], recv_sem=yr_sem.at[blk, zz],
            device_id={"dev": across}, device_id_type=MESH)

    def z_copy(blk, zz, src):
        rows = pl.ds(zz * (OCC * QBLK), OCC * QBLK)
        return pltpu.make_async_remote_copy(
            src_ref=e_buf.at[y, blk, rows], dst_ref=e_all.at[src * BLKS + blk],
            send_sem=zs_sem.at[blk, zz], recv_sem=zr_sem.at[blk, src],
            device_id={"dev2": zz}, device_id_type=MESH)

    barrier = pltpu.get_barrier_semaphore()
    for peer in ({"dev": sib}, {"dev": across}, {"dev2": (z + 1) % 4}, {"dev2": (z + 2) % 4}, {"dev2": (z + 3) % 4}):
        pl.semaphore_signal(barrier, inc=1, device_id=peer, device_id_type=MESH)

    for s in range(AHEAD):
        a_copy(s).start()

    occ = occ_ref[...]
    row = iota((OCC, OCC), 0)
    perm = select(iota((OCC, OCC), 1) == 3 * (row % 8) + row // 8)
    occ_t = dot_nt(perm, occ).astype(BF16)
    zero = jnp.zeros((OCC, 128), BF16)
    occ_lhs[...] = jnp.concatenate(
        [jnp.concatenate([occ_t, zero], 1), jnp.concatenate([zero, occ_t], 1)], 0)
    virt = virt_ref[...]
    col = iota((VIRT, 256), 1)
    lane = col % 128
    pair = (col // 128) * LANES + lane
    for jj in range(3):
        pick = select((pair == jj * VIRT + iota((VIRT, 256), 0)) & (lane < LANES))
        virt_rhs[pl.ds(jj * 128, 128), :] = dot(virt, pick).astype(BF16)
    row = iota((192, OCC), 0)
    pick_i = select(row % OCC == iota((192, OCC), 1))
    pick_p = select(iota((32, 256), 1) // 8 == iota((32, 256), 0))
    row = iota((192, 256), 0)
    keep = iota((192, 256), 1) % 8 == 2 * ((row % 96) // OCC) + row // 96
    for dst, who in ((kron_own, dev), (kron_sib, sib)):
        part = dot_nt(pick_i, occ_ref[pl.ds(pl.multiple_of(who * 32, 32), 32), :]).astype(BF16)
        dst[...] = jnp.where(keep, dot(part, pick_p), 0.0).astype(BF16)
    eye = select(iota((VIRT, VIRT), 0) == iota((VIRT, VIRT), 1))
    virt_t[...] = dot_nt(eye, virt).astype(BF16)

    pl.semaphore_wait(barrier, 5)

    def half_step(s):
        for qq in range(QSUB):
            rows = []
            for p in range(0, 32, 4):
                a = [a_buf[s, p + k, qq] for k in range(4)]
                w = jnp.concatenate(
                    [jnp.concatenate(a[:2], 1), jnp.concatenate(a[2:], 1)], 0)
                r = dot(occ_lhs[...], w)
                for k in range(4):
                    part = r[(k // 2) * OCC:(k // 2 + 1) * OCC, (k % 2) * 128:(k % 2 + 1) * 128]
                    rows.append(jnp.concatenate([part[0:8], part[8:16], part[16:24]], 1))
            t_one = jnp.concatenate(rows, 0).astype(BF16)
            h = dot(t_one, virt_rhs[...]).astype(BF16)
            h_buf[0, s * QSUB + qq] = h[:, :128]
            h_buf[1, s * QSUB + qq] = h[:, 128:]

    def e_step(s):
        q = s * QSUB
        own = jnp.concatenate([h_buf[core, q + k] for k in range(QSUB)], 1)
        other = jnp.concatenate([h_in[q + k] for k in range(QSUB)], 1)
        e = dot(kron_own[...], own) + dot(kron_sib[...], other)
        blk = s // SUBS
        for k in range(QSUB):
            for yy in range(2):
                e_buf[yy, blk, pl.ds((s % SUBS) * QSUB + k, 96, stride=QBLK), :] = (
                    e[yy * 96:(yy + 1) * 96, k * 128:(k + 1) * 128])

    def step(s, carry):
        @pl.when(s < STEPS)
        def _():
            a_copy(s).wait()

            @pl.when(s + AHEAD < STEPS)
            def _():
                a_copy(s + AHEAD).start()
            half_step(s)
            h_copy(s).start()

        @pl.when(s > 0)
        def _():
            h_copy(s - 1).wait_recv()
            e_step(s - 1)

            @pl.when((s - 1) % SUBS == SUBS - 1)
            def _():
                for zz in (*order, z):
                    y_copy((s - 1) // SUBS, zz).start()
        return carry

    lax.fori_loop(0, STEPS + 1, step, 0)

    def sum_step(blk, carry):
        for zz in order:
            rows = pl.ds(pl.multiple_of(zz * (OCC * QBLK), 8), OCC * QBLK)
            y_copy(blk, zz).wait_recv()
            e_buf[y, blk, rows] = e_buf[y, blk, rows] + y_in[blk, rows]
            z_copy(blk, zz, z).start()
        rows = pl.ds(pl.multiple_of(z * (OCC * QBLK), 8), OCC * QBLK)
        y_copy(blk, z).wait_recv()
        e_all[z * BLKS + blk] = e_buf[y, blk, rows] + y_in[blk, rows]
        return carry

    lax.fori_loop(0, BLKS, sum_step, 0)

    def arrived(blk, carry):
        for d in range(1, 4):
            z_copy(blk, z, (z + d) % 4).wait_recv()
        return carry

    lax.fori_loop(0, BLKS, arrived, 0)

    def v_step(n, carry):
        for pr in range(2):
            parts = []
            for k in range(2):
                i = n * 4 + pr * 2 + k
                e = e_all[:, pl.ds(pl.multiple_of(i * QBLK, 8), QBLK), :].reshape(128, 128)
                hi = e.astype(BF16)
                rest = e - hi.astype(F32)
                mid = rest.astype(BF16)
                low = (rest - mid.astype(F32)).astype(BF16)
                parts.append((hi, mid, low))
            v = jnp.zeros((VIRT, 256), F32)
            for a, b in zip(*parts):
                v = v + dot(virt_t[...], jnp.concatenate([a, b], 1))
            for k in range(2):
                out_ref[n * 4 + pr * 2 + k] = v[:, k * 128:k * 128 + LANES]
        return carry

    lax.fori_loop(0, OCC // 4, v_step, 0)

    def sent(s, carry):
        h_copy(s).wait_send()
        return carry

    lax.fori_loop(0, STEPS, sent, 0)

    def sent_blk(blk, carry):
        for zz in (*order, z):
            y_copy(blk, zz).wait_send()
        for zz in order:
            z_copy(blk, zz, z).wait_send()
        return carry

    lax.fori_loop(0, BLKS, sent_blk, 0)


def solution(mesh):
    def local_block(ao_blk, c_occ, c_virt):
        vmem = pl.BlockSpec(memory_space=pltpu.VMEM)
        return pl.pallas_call(
            kernel,
            out_shape=jax.ShapeDtypeStruct((OCC, VIRT, LANES), F32),
            in_specs=[pl.BlockSpec(memory_space=pl.ANY), vmem, vmem],
            out_specs=vmem,
            scratch_shapes=[
                pltpu.VMEM((STEPS, 32, QSUB, 128, 128), BF16),
                pltpu.VMEM((2 * OCC, 256), BF16),
                pltpu.VMEM((384, 256), BF16),
                pltpu.VMEM((192, 256), BF16),
                pltpu.VMEM((192, 256), BF16),
                pltpu.VMEM((VIRT, 128), BF16),
                pltpu.VMEM((2, 32, 256, 128), BF16),
                pltpu.VMEM((32, 256, 128), BF16),
                pltpu.VMEM((2, BLKS, 4 * OCC * QBLK, 128), F32),
                pltpu.VMEM((BLKS, 4 * OCC * QBLK, 128), F32),
                pltpu.VMEM((4 * BLKS, OCC * QBLK, 128), F32),
                pltpu.SemaphoreType.DMA((STEPS,)),
                pltpu.SemaphoreType.DMA((STEPS,)),
                pltpu.SemaphoreType.DMA((STEPS,)),
                pltpu.SemaphoreType.DMA((BLKS, 4)),
                pltpu.SemaphoreType.DMA((BLKS, 4)),
                pltpu.SemaphoreType.DMA((BLKS, 4)),
                pltpu.SemaphoreType.DMA((BLKS, 4)),
            ],
            compiler_params=pltpu.CompilerParams(
                collective_id=0, has_side_effects=True, vmem_limit_bytes=60 * 1024 * 1024),
        )(ao_blk, c_occ, c_virt)

    return jax.shard_map(
        local_block, mesh=mesh,
        in_specs=(P(("frag", "dev"), "dev2", None, None), P("frag", None), P("frag", None)),
        out_specs=P("frag", None, ("dev2", "dev")),
        check_vma=False)
```

```python
import functools

import jax
import jax.numpy as jnp
from jax import lax
from jax.experimental import pallas as pl
from jax.experimental.pallas import tpu as pltpu
from jax.sharding import PartitionSpec as P

MESH = pl.DeviceIdType.MESH
F32 = jnp.float32
BF16 = jnp.bfloat16
OCC = 24
VIRT = 80
LANES = 120
QSUB = 2
QBLK = 4
STEPS = 32 // QSUB
BLKS = 32 // QBLK
SUBS = QBLK // QSUB
SLOTS = 8
AHEAD = 6
LAG = 3


def dot(a, b):
    return jnp.dot(a, b, preferred_element_type=F32)


def dot_nt(a, b):
    return lax.dot_general(a, b, (((1,), (1,)), ((), ())), preferred_element_type=F32)


def iota(shape, dim):
    return lax.broadcasted_iota(jnp.int32, shape, dim)


def select(mask):
    return jnp.where(mask, 1.0, 0.0).astype(BF16)


def kernel(ao_ref, occ_ref, virt_ref, out_ref,
           a_buf, occ_lhs, virt_rhs, kron_own, kron_sib,
           h_buf, h_in, e_buf, y_in, e_all,
           a_sem, hs_sem, hr_sem, ys_sem, yr_sem, zs_sem, zr_sem):
    z = lax.axis_index("dev2")
    dev = lax.axis_index("dev")
    y = dev // 2
    core = dev % 2
    sib = y * 2 + (1 - core)
    across = (1 - y) * 2 + core
    half = z // 2
    order = (3 * (1 - half), 2 - half, 1 - z + 4 * half)

    def e_rows(blk, zz):
        return pl.ds(pl.multiple_of((zz * 32 + blk * QBLK) * OCC, 8), OCC * QBLK)

    def a_copy(s):
        return pltpu.make_async_copy(
            ao_ref.at[:, pl.ds(s * QSUB, QSUB)], a_buf.at[s % SLOTS], a_sem.at[s])

    def h_copy(s):
        return pltpu.make_async_remote_copy(
            src_ref=h_buf.at[1 - core, pl.ds(s * QSUB, QSUB)],
            dst_ref=h_in.at[pl.ds(s * QSUB, QSUB)],
            send_sem=hs_sem.at[s], recv_sem=hr_sem.at[s],
            device_id={"dev": sib}, device_id_type=MESH)

    def y_copy(blk, zz):
        return pltpu.make_async_remote_copy(
            src_ref=e_buf.at[1 - y, e_rows(blk, zz)], dst_ref=y_in.at[e_rows(blk, zz)],
            send_sem=ys_sem.at[blk, zz], recv_sem=yr_sem.at[blk, zz],
            device_id={"dev": across}, device_id_type=MESH)

    def z_copy(blk, zz, src):
        return pltpu.make_async_remote_copy(
            src_ref=e_buf.at[y, e_rows(blk, zz)], dst_ref=e_all.at[e_rows(blk, src)],
            send_sem=zs_sem.at[blk, zz], recv_sem=zr_sem.at[blk, src],
            device_id={"dev2": zz}, device_id_type=MESH)

    barrier = pltpu.get_barrier_semaphore()
    for peer in ({"dev": sib}, {"dev": across}, {"dev2": (z + 1) % 4}, {"dev2": (z + 2) % 4}, {"dev2": (z + 3) % 4}):
        pl.semaphore_signal(barrier, inc=1, device_id=peer, device_id_type=MESH)

    for s in range(AHEAD):
        a_copy(s).start()

    row = iota((OCC, OCC), 0)
    perm = select(iota((OCC, OCC), 1) == 3 * (row % 8) + row // 8)
    occ_t = dot(perm, occ_ref[...]).astype(BF16)
    zero = jnp.zeros((OCC, 128), BF16)
    occ_lhs[...] = jnp.concatenate(
        [jnp.concatenate([occ_t, zero], 1), jnp.concatenate([zero, occ_t], 1)], 0)
    row = iota((256, VIRT), 0)
    lane = row % 128
    pair = (row // 128) * LANES + lane
    for jj in range(3):
        pick = select((pair == jj * VIRT + iota((256, VIRT), 1)) & (lane < LANES))
        virt_rhs[:, pl.ds(jj * 128, 128)] = dot(pick, virt_ref[...]).astype(BF16)
    row = iota((192, OCC), 0)
    pick_i = select(row % OCC == iota((192, OCC), 1))
    occ_i = dot(pick_i, occ_ref[...]).astype(BF16)
    row = iota((192, 256), 0)
    keep = iota((192, 256), 1) % 8 == 2 * ((row % 96) // OCC) + row // 96
    for dst, who in ((kron_own, dev), (kron_sib, sib)):
        pick_p = select(iota((128, 256), 1) // 8 + who * 32 == iota((128, 256), 0))
        dst[...] = jnp.where(keep, dot(occ_i, pick_p), 0.0).astype(BF16)

    def half_step(s):
        for qq in range(QSUB):
            rows = []
            for p in range(0, 32, 4):
                a = [a_buf[s % SLOTS, p + k, qq] for k in range(4)]
                w = jnp.concatenate(
                    [jnp.concatenate(a[:2], 1), jnp.concatenate(a[2:], 1)], 0)
                r = dot(occ_lhs[...], w)
                for k in range(4):
                    part = r[(k // 2) * OCC:(k // 2 + 1) * OCC, (k % 2) * 128:(k % 2 + 1) * 128]
                    rows.append(jnp.concatenate([part[0:8], part[8:16], part[16:24]], 1))
            t_one = jnp.concatenate(rows, 0).astype(BF16)
            h = dot_nt(t_one, virt_rhs[...]).astype(BF16)
            h_buf[0, s * QSUB + qq] = h[:, :128]
            h_buf[1, s * QSUB + qq] = h[:, 128:]

    def e_step(s):
        q = s * QSUB
        own = jnp.concatenate([h_buf[core, q + k] for k in range(QSUB)], 1)
        other = jnp.concatenate([h_in[q + k] for k in range(QSUB)], 1)
        e = dot(kron_own[...], own) + dot(kron_sib[...], other)
        for k in range(QSUB):
            for yy in range(2):
                for zz in range(4):
                    r = (yy * 4 + zz) * OCC
                    e_buf[yy, pl.ds(pl.multiple_of((zz * 32 + q + k) * OCC, 8), OCC), :] = (
                        e[r:r + OCC, k * 128:(k + 1) * 128])

    def sum_block(blk):
        for zz in order:
            y_copy(blk, zz).wait_recv()
            rows = e_rows(blk, zz)
            e_buf[y, rows] = e_buf[y, rows] + y_in[rows]
            z_copy(blk, zz, z).start()
        y_copy(blk, z).wait_recv()
        rows = e_rows(blk, z)
        e_all[rows] = e_buf[y, rows] + y_in[rows]

    def step(s, carry):
        @pl.when(s < STEPS)
        def _():
            a_copy(s).wait()

            @pl.when(s + AHEAD < STEPS)
            def _():
                a_copy(s + AHEAD).start()
            half_step(s)

            @pl.when(s == 0)
            def _():
                pl.semaphore_wait(barrier, 5)
            h_copy(s).start()

        @pl.when((s > 0) & (s <= STEPS))
        def _():
            h_copy(s - 1).wait_recv()
            e_step(s - 1)

            @pl.when(s % SUBS == 0)
            def _():
                for zz in (*order, z):
                    y_copy(s // SUBS - 1, zz).start()

        @pl.when((s % SUBS == SUBS - 1) & (s // SUBS >= LAG))
        def _():
            sum_block(s // SUBS - LAG)
        return carry

    lax.fori_loop(0, STEPS + LAG * SUBS, step, 0)

    def arrived(blk, carry):
        for d in range(1, 4):
            z_copy(blk, z, (z + d) % 4).wait_recv()
        return carry

    lax.fori_loop(0, BLKS, arrived, 0)

    def v_step(n, carry):
        for pr in range(2):
            parts = []
            for k in range(2):
                i = n * 4 + pr * 2 + k
                e = e_all[pl.ds(i, 128, stride=OCC), :]
                hi = e.astype(BF16)
                rest = e - hi.astype(F32)
                mid = rest.astype(BF16)
                low = (rest - mid.astype(F32)).astype(BF16)
                parts.append((hi, mid, low))
            v = jnp.zeros((VIRT, 256), F32)
            for a, b in zip(*parts):
                v = v + dot(virt_ref[...], jnp.concatenate([a, b], 1))
            for k in range(2):
                out_ref[n * 4 + pr * 2 + k] = v[:, k * 128:k * 128 + LANES]
        return carry

    lax.fori_loop(0, OCC // 4, v_step, 0)

    def sent(s, carry):
        h_copy(s).wait_send()
        return carry

    lax.fori_loop(0, STEPS, sent, 0)

    def sent_blk(blk, carry):
        for zz in (*order, z):
            y_copy(blk, zz).wait_send()
        for zz in order:
            z_copy(blk, zz, z).wait_send()
        return carry

    lax.fori_loop(0, BLKS, sent_blk, 0)


def solution(mesh):
    def local_block(ao_blk, c_occ, c_virt):
        vmem = pl.BlockSpec(memory_space=pltpu.VMEM)
        return pl.pallas_call(
            kernel,
            out_shape=jax.ShapeDtypeStruct((OCC, VIRT, LANES), F32),
            in_specs=[pl.BlockSpec(memory_space=pl.ANY), vmem, vmem],
            out_specs=vmem,
            scratch_shapes=[
                pltpu.VMEM((SLOTS, 32, QSUB, 128, 128), BF16),
                pltpu.VMEM((2 * OCC, 256), BF16),
                pltpu.VMEM((256, 384), BF16),
                pltpu.VMEM((192, 256), BF16),
                pltpu.VMEM((192, 256), BF16),
                pltpu.VMEM((2, 32, 256, 128), BF16),
                pltpu.VMEM((32, 256, 128), BF16),
                pltpu.VMEM((2, 4 * 32 * OCC, 128), F32),
                pltpu.VMEM((4 * 32 * OCC, 128), F32),
                pltpu.VMEM((128 * OCC, 128), F32),
                pltpu.SemaphoreType.DMA((STEPS,)),
                pltpu.SemaphoreType.DMA((STEPS,)),
                pltpu.SemaphoreType.DMA((STEPS,)),
                pltpu.SemaphoreType.DMA((BLKS, 4)),
                pltpu.SemaphoreType.DMA((BLKS, 4)),
                pltpu.SemaphoreType.DMA((BLKS, 4)),
                pltpu.SemaphoreType.DMA((BLKS, 4)),
            ],
            compiler_params=pltpu.CompilerParams(
                collective_id=0, has_side_effects=True, vmem_limit_bytes=36 * 1024 * 1024),
        )(ao_blk, c_occ.T, c_virt.T)

    return jax.shard_map(
        local_block, mesh=mesh,
        in_specs=(P(("frag", "dev"), "dev2", None, None), P("frag", None), P("frag", None)),
        out_specs=P("frag", None, ("dev2", "dev")),
        check_vma=False)
```

```python
import functools

import jax
import jax.numpy as jnp
from jax import lax
from jax.experimental import pallas as pl
from jax.experimental.pallas import tpu as pltpu
from jax.sharding import PartitionSpec as P

MESH = pl.DeviceIdType.MESH
F32 = jnp.float32
BF16 = jnp.bfloat16
OCC = 24
VIRT = 80
LANES = 120
QSUB = 2
QBLK = 4
STEPS = 32 // QSUB
BLKS = 32 // QBLK
SUBS = QBLK // QSUB
SLOTS = 8
AHEAD = 6
LAG = 2


def dot(a, b):
    return jnp.dot(a, b, preferred_element_type=F32)


def dot_nt(a, b):
    return lax.dot_general(a, b, (((1,), (1,)), ((), ())), preferred_element_type=F32)


def iota(shape, dim):
    return lax.broadcasted_iota(jnp.int32, shape, dim)


def select(mask):
    return jnp.where(mask, 1.0, 0.0).astype(BF16)


def kernel(ao_ref, occ_hbm, virt_hbm, out_ref,
           a_buf, occ_lhs, virt_rhs, kron_own, kron_sib,
           h_buf, h_in, e_buf, y_in, e_all,
           a_sem, hs_sem, hr_sem, ys_sem, yr_sem, zs_sem, zr_sem, c_sem, occ_ref, virt_ref):
    z = lax.axis_index("dev2")
    dev = lax.axis_index("dev")
    y = dev // 2
    core = dev % 2
    sib = y * 2 + (1 - core)
    across = (1 - y) * 2 + core
    half = z // 2
    order = (3 * (1 - half), 2 - half, 1 - z + 4 * half)

    def e_rows(blk, zz):
        return pl.ds(pl.multiple_of((zz * 32 + blk * QBLK) * OCC, 8), OCC * QBLK)

    def a_copy(s):
        return pltpu.make_async_copy(
            ao_ref.at[:, pl.ds(s * QSUB, QSUB)], a_buf.at[s % SLOTS], a_sem.at[s % SLOTS])

    def h_copy(s):
        return pltpu.make_async_remote_copy(
            src_ref=h_buf.at[1 - core, pl.ds(s * QSUB, QSUB)],
            dst_ref=h_in.at[pl.ds(s * QSUB, QSUB)],
            send_sem=hs_sem, recv_sem=hr_sem.at[s],
            device_id={"dev": sib}, device_id_type=MESH)

    def y_copy(blk, zz):
        return pltpu.make_async_remote_copy(
            src_ref=e_buf.at[1 - y, e_rows(blk, zz)], dst_ref=y_in.at[e_rows(blk, zz)],
            send_sem=ys_sem, recv_sem=yr_sem.at[blk, zz],
            device_id={"dev": across}, device_id_type=MESH)

    def z_copy(blk, zz, src):
        return pltpu.make_async_remote_copy(
            src_ref=e_buf.at[y, e_rows(blk, zz)], dst_ref=e_all.at[e_rows(blk, src)],
            send_sem=zs_sem, recv_sem=zr_sem,
            device_id={"dev2": zz}, device_id_type=MESH)

    barrier = pltpu.get_barrier_semaphore()
    for peer in ({"dev": sib}, {"dev": across}, {"dev2": (z + 1) % 4}, {"dev2": (z + 2) % 4}, {"dev2": (z + 3) % 4}):
        pl.semaphore_signal(barrier, inc=1, device_id=peer, device_id_type=MESH)

    c_copies = (pltpu.make_async_copy(occ_hbm, occ_ref, c_sem.at[0]), pltpu.make_async_copy(virt_hbm, virt_ref, c_sem.at[1]))
    for c in c_copies:
        c.start()
    for s in range(AHEAD):
        a_copy(s).start()
    for c in c_copies:
        c.wait()

    row = iota((OCC, OCC), 0)
    perm = select(iota((OCC, OCC), 1) == 3 * (row % 8) + row // 8)
    occ_t = dot(perm, occ_ref[...]).astype(BF16)
    zero = jnp.zeros((OCC, 128), BF16)
    occ_lhs[...] = jnp.concatenate(
        [jnp.concatenate([occ_t, zero], 1), jnp.concatenate([zero, occ_t], 1)], 0)
    row = iota((256, VIRT), 0)
    lane = row % 128
    pair = (row // 128) * LANES + lane
    for jj in range(3):
        pick = select((pair == jj * VIRT + iota((256, VIRT), 1)) & (lane < LANES))
        virt_rhs[:, pl.ds(jj * 128, 128)] = dot(pick, virt_ref[...]).astype(BF16)
    row = iota((192, OCC), 0)
    pick_i = select(row % OCC == iota((192, OCC), 1))
    occ_i = dot(pick_i, occ_ref[...]).astype(BF16)
    row = iota((192, 256), 0)
    keep = iota((192, 256), 1) % 8 == 2 * ((row % 96) // OCC) + row // 96
    for dst, who in ((kron_own, dev), (kron_sib, sib)):
        pick_p = select(iota((128, 256), 1) // 8 + who * 32 == iota((128, 256), 0))
        dst[...] = jnp.where(keep, dot(occ_i, pick_p), 0.0).astype(BF16)

    def half_step(s):
        for qq in range(QSUB):
            rows = []
            for p in range(0, 32, 4):
                a = [a_buf[s % SLOTS, p + k, qq] for k in range(4)]
                w = jnp.concatenate(
                    [jnp.concatenate(a[:2], 1), jnp.concatenate(a[2:], 1)], 0)
                r = dot(occ_lhs[...], w)
                for k in range(4):
                    part = r[(k // 2) * OCC:(k // 2 + 1) * OCC, (k % 2) * 128:(k % 2 + 1) * 128]
                    rows.append(jnp.concatenate([part[0:8], part[8:16], part[16:24]], 1))
            t_one = jnp.concatenate(rows, 0).astype(BF16)
            h = dot_nt(t_one, virt_rhs[...]).astype(BF16)
            h_buf[0, s * QSUB + qq] = h[:, :128]
            h_buf[1, s * QSUB + qq] = h[:, 128:]

    def e_step(s):
        q = s * QSUB
        own = jnp.concatenate([h_buf[core, q + k] for k in range(QSUB)], 1)
        other = jnp.concatenate([h_in[q + k] for k in range(QSUB)], 1)
        e = dot(kron_own[...], own) + dot(kron_sib[...], other)
        for k in range(QSUB):
            for yy in range(2):
                for zz in range(4):
                    r = (yy * 4 + zz) * OCC
                    e_buf[yy, pl.ds(pl.multiple_of((zz * 32 + q + k) * OCC, 8), OCC), :] = (
                        e[r:r + OCC, k * 128:(k + 1) * 128])

    def sum_block(blk):
        for zz in order:
            y_copy(blk, zz).wait_recv()
            rows = e_rows(blk, zz)
            e_buf[y, rows] = e_buf[y, rows] + y_in[rows]
            z_copy(blk, zz, z).start()
        y_copy(blk, z).wait_recv()
        rows = e_rows(blk, z)
        e_all[rows] = e_buf[y, rows] + y_in[rows]

    def step(s, carry):
        @pl.when(s < STEPS)
        def _():
            a_copy(s).wait()

            @pl.when(s + AHEAD < STEPS)
            def _():
                a_copy(s + AHEAD).start()
            half_step(s)

            @pl.when(s == 0)
            def _():
                pl.semaphore_wait(barrier, 5)
            h_copy(s).start()

        @pl.when((s > 0) & (s <= STEPS))
        def _():
            h_copy(s - 1).wait_recv()
            e_step(s - 1)

            @pl.when(s % SUBS == 0)
            def _():
                for zz in (*order, z):
                    y_copy(s // SUBS - 1, zz).start()

        @pl.when((s % SUBS == SUBS - 1) & (s // SUBS >= LAG))
        def _():
            sum_block(s // SUBS - LAG)
        return carry

    lax.fori_loop(0, STEPS + LAG * SUBS, step, 0)

    part = pl.ds(0, 3 * 32 * OCC)
    arrivals = pltpu.make_async_remote_copy(
        src_ref=e_buf.at[y, part], dst_ref=e_all.at[part], send_sem=zs_sem, recv_sem=zr_sem,
        device_id={"dev2": (z + 1) % 4}, device_id_type=MESH)
    arrivals.wait_recv()

    def v_step(n, carry):
        for pr in range(2):
            parts = []
            for k in range(2):
                i = n * 4 + pr * 2 + k
                e = e_all[pl.ds(i, 128, stride=OCC), :]
                hi = e.astype(BF16)
                rest = e - hi.astype(F32)
                mid = rest.astype(BF16)
                low = (rest - mid.astype(F32)).astype(BF16)
                parts.append((hi, mid, low))
            v = jnp.zeros((VIRT, 256), F32)
            for a, b in zip(*parts):
                v = v + dot(virt_ref[...], jnp.concatenate([a, b], 1))
            for k in range(2):
                out_ref[n * 4 + pr * 2 + k] = v[:, k * 128:k * 128 + LANES]
        return carry

    lax.fori_loop(0, OCC // 4, v_step, 0)

    pltpu.make_async_remote_copy(
        src_ref=h_buf.at[1 - core], dst_ref=h_in, send_sem=hs_sem, recv_sem=hr_sem.at[0],
        device_id={"dev": sib}, device_id_type=MESH).wait_send()
    pltpu.make_async_remote_copy(
        src_ref=e_buf.at[1 - y], dst_ref=y_in, send_sem=ys_sem, recv_sem=yr_sem.at[0, 0],
        device_id={"dev": across}, device_id_type=MESH).wait_send()
    arrivals.wait_send()


def solution(mesh):
    def local_block(ao_blk, c_occ, c_virt):
        vmem = pl.BlockSpec(memory_space=pltpu.VMEM)
        return pl.pallas_call(
            kernel,
            out_shape=jax.ShapeDtypeStruct((OCC, VIRT, LANES), F32),
            in_specs=[pl.BlockSpec(memory_space=pltpu.HBM)] * 3,
            out_specs=vmem,
            scratch_shapes=[
                pltpu.VMEM((SLOTS, 32, QSUB, 128, 128), BF16),
                pltpu.VMEM((2 * OCC, 256), BF16),
                pltpu.VMEM((256, 384), BF16),
                pltpu.VMEM((192, 256), BF16),
                pltpu.VMEM((192, 256), BF16),
                pltpu.VMEM((2, 32, 256, 128), BF16),
                pltpu.VMEM((32, 256, 128), BF16),
                pltpu.VMEM((2, 4 * 32 * OCC, 128), F32),
                pltpu.VMEM((4 * 32 * OCC, 128), F32),
                pltpu.VMEM((128 * OCC, 128), F32),
                pltpu.SemaphoreType.DMA((SLOTS,)),
                pltpu.SemaphoreType.DMA,
                pltpu.SemaphoreType.DMA((STEPS,)),
                pltpu.SemaphoreType.DMA,
                pltpu.SemaphoreType.DMA((BLKS, 4)),
                pltpu.SemaphoreType.DMA,
                pltpu.SemaphoreType.DMA,
                pltpu.SemaphoreType.DMA((2,)),
                pltpu.VMEM((OCC, 128), BF16),
                pltpu.VMEM((VIRT, 128), BF16),
            ],
            compiler_params=pltpu.CompilerParams(
                collective_id=0, has_side_effects=True, vmem_limit_bytes=36 * 1024 * 1024),
        )(ao_blk, c_occ.T, c_virt.T)

    return jax.shard_map(
        local_block, mesh=mesh,
        in_specs=(P(("frag", "dev"), "dev2", None, None), P("frag", None), P("frag", None)),
        out_specs=P("frag", None, ("dev2", "dev")),
        check_vma=False)
```

```python
import functools

import jax
import jax.numpy as jnp
from jax import lax
from jax.experimental import pallas as pl
from jax.experimental.pallas import tpu as pltpu
from jax.sharding import PartitionSpec as P

MESH = pl.DeviceIdType.MESH
F32 = jnp.float32
BF16 = jnp.bfloat16
OCC = 24
VIRT = 80
LANES = 120
SPECIAL = 2
KEPT = 32 - SPECIAL
RIDERS = KEPT // SPECIAL
FREE = 128 - LANES
PART = 32 * OCC
STEPS = 17
LATE = 7
SLOTS = 16
AHEAD = 6
QGRP = 8
GROUPS = 4
H_RING = 4
Y_RING = 8
CHUNKS = ((0, 8), (8, 8), (16, 8), (24, 6))
CROSS_SUM = 4
NEAR_AT = (10, 13, 16, 18)
NEAR_SUM = (14, 17, 20, 22)
OWN_AT = (14, 17, 19, 20)
V_AT = (18, 21, 24)
END = 25


def dot(a, b):
    return jnp.dot(a, b, preferred_element_type=F32)


def dot_nt(a, b):
    return lax.dot_general(a, b, (((1,), (1,)), ((), ())), preferred_element_type=F32)


def iota(shape, dim):
    return lax.broadcasted_iota(jnp.int32, shape, dim)


def select(mask):
    return jnp.where(mask, 1.0, 0.0).astype(BF16)


def kernel(ao_ref, occ_hbm, virt_hbm, out_ref,
           a_buf, a_late, occ_lhs, virt_rhs, kron_own, kron_sib, virt_v,
           h_buf, h_in, e_special, e_buf, y_in, e_all, occ_ref, virt_ref,
           c_sem, a_sem, al_sem, hs_sem, hr_sem, hl_sem, ys_sem, yc_sem, yn_sem, yo_sem,
           zs_sem, zc_sem, zn_sem):
    z = lax.axis_index("dev2")
    dev = lax.axis_index("dev")
    y = dev // 2
    core = dev % 2
    sib = y * 2 + (1 - core)
    across = (1 - y) * 2 + core
    half = z // 2
    far = 3 * (1 - half)
    far_near = 2 - half
    near = 1 - z + 4 * half

    def rows_of(q, n):
        if not isinstance(q, int):
            q = pl.multiple_of(q * OCC, 8)
        else:
            q = q * OCC
        return pl.ds(q, n * OCC)

    def a_copy(q, n, s):
        return pltpu.make_async_copy(
            ao_ref.at[:, pl.ds(q, n)], a_buf.at[:, pl.ds(q % SLOTS, n)], a_sem.at[s % 8])

    a_copy_late = pltpu.make_async_copy(ao_ref.at[:, 31], a_late, al_sem)

    def h_copy(q, n, sem):
        return pltpu.make_async_remote_copy(
            src_ref=h_buf.at[1 - core, pl.ds(q, n)], dst_ref=h_in.at[pl.ds(q, n)],
            send_sem=hs_sem, recv_sem=sem,
            device_id={"dev": sib}, device_id_type=MESH)

    def y_copy(z0, zn, q, n, sem):
        return pltpu.make_async_remote_copy(
            src_ref=e_buf.at[1 - y, pl.ds(z0, zn), rows_of(q, n)],
            dst_ref=y_in.at[pl.ds(z0, zn), rows_of(q, n)],
            send_sem=ys_sem, recv_sem=sem,
            device_id={"dev": across}, device_id_type=MESH)

    def y_cross(q, n, s):
        return y_copy(2 * (1 - half), 2, q, n, yc_sem.at[s % Y_RING])

    def y_near(k):
        return y_copy(near, 1, *CHUNKS[k], yn_sem.at[k])

    def y_own(k):
        return y_copy(z, 1, *CHUNKS[k], yo_sem.at[k])

    def add_send(zz, q, n, sem):
        rows = rows_of(q, n)
        e_buf[y, zz, rows] = e_buf[y, zz, rows] + y_in[zz, rows]
        pltpu.make_async_remote_copy(
            src_ref=e_buf.at[y, zz, rows], dst_ref=e_all.at[rows_of(z * 32 + q, n)],
            send_sem=zs_sem, recv_sem=sem,
            device_id={"dev2": zz}, device_id_type=MESH).start()

    def z_wait(n, sem):
        rows = pl.ds(0, n * OCC)
        pltpu.make_async_remote_copy(
            src_ref=e_all.at[rows], dst_ref=e_all.at[rows], send_sem=zs_sem, recv_sem=sem,
            device_id={"dev2": near}, device_id_type=MESH).wait_recv()

    def when_step(s, first, end, shift, do):
        t = s - shift

        if first == 0:
            @pl.when(t == 0)
            def _():
                do(30, 1, 0)

        @pl.when((t == 1) | (t == 2))
        def _():
            do(t - 1, 1, t)

        @pl.when((t > 2) & (t < end))
        def _():
            do(2 * t - 4, 2, t)

    barrier = pltpu.get_barrier_semaphore()
    for peer in ({"dev": sib}, {"dev": across}, {"dev2": (z + 1) % 4}, {"dev2": (z + 2) % 4}, {"dev2": (z + 3) % 4}):
        pl.semaphore_signal(barrier, inc=1, device_id=peer, device_id_type=MESH)

    c_copies = (pltpu.make_async_copy(occ_hbm, occ_ref, c_sem.at[0]),
                pltpu.make_async_copy(virt_hbm, virt_ref, c_sem.at[1]))
    for c in c_copies:
        c.start()
    a_copy(30, 1, 0).start()
    for i in range(OCC):
        out_ref[i] = jnp.zeros((VIRT, LANES), F32)
    for c in c_copies:
        c.wait()
    for s in range(1, AHEAD):
        a_copy(*((s - 1, 1) if s < 3 else (2 * s - 4, 2)), s).start()

    row = iota((OCC, OCC), 0)
    perm = select(iota((OCC, OCC), 1) == 3 * (row % 8) + row // 8)
    occ_t = dot(perm, occ_ref[...]).astype(BF16)
    zero = jnp.zeros((OCC, 128), BF16)
    occ_lhs[...] = jnp.concatenate(
        [jnp.concatenate([occ_t, zero], 1), jnp.concatenate([zero, occ_t], 1)], 0)
    row = iota((256, VIRT), 0)
    lane = row % 128
    pair = (row // 128) * LANES + lane
    for jj in range(3):
        pick = select((pair == jj * VIRT + iota((256, VIRT), 1)) & (lane < LANES))
        virt_rhs[:, pl.ds(jj * 128, 128)] = dot(pick, virt_ref[...]).astype(BF16)
    row = iota((192, OCC), 0)
    pick_i = select(row % OCC == iota((192, OCC), 1))
    occ_i = dot(pick_i, occ_ref[...]).astype(BF16)
    row = iota((192, 256), 0)
    keep = iota((192, 256), 1) % 8 == 2 * ((row % 96) // OCC) + row // 96
    for dst, who in ((kron_own, dev), (kron_sib, sib)):
        pick_p = select(iota((128, 256), 1) // 8 + who * 32 == iota((128, 256), 0))
        dst[...] = jnp.where(keep, dot(occ_i, pick_p), 0.0).astype(BF16)
    col = iota((128, 96), 1)
    for g in range(GROUPS):
        pick_q = select(iota((128, 96), 0) == (col % 32) // QGRP * 32 + g * QGRP + col % QGRP)
        virt_v[g] = dot(virt_ref[...], pick_q).astype(BF16)

    def half_step(tiles, q, n):
        for qq in range(n):
            rows = []
            for p in range(0, 32, 4):
                a = [tiles(p + k, qq) for k in range(4)]
                w = jnp.concatenate(
                    [jnp.concatenate(a[:2], 1), jnp.concatenate(a[2:], 1)], 0)
                r = dot(occ_lhs[...], w)
                for k in range(4):
                    part = r[(k // 2) * OCC:(k // 2 + 1) * OCC, (k % 2) * 128:(k % 2 + 1) * 128]
                    rows.append(jnp.concatenate([part[0:8], part[8:16], part[16:24]], 1))
            t_one = jnp.concatenate(rows, 0).astype(BF16)
            h = dot_nt(t_one, virt_rhs[...]).astype(BF16)
            h_buf[0, q + qq] = h[:, :128]
            h_buf[1, q + qq] = h[:, 128:]

    def contract_p(q, n):
        own = jnp.concatenate([h_buf[core, q + k] for k in range(n)], 1)
        other = jnp.concatenate([h_in[q + k] for k in range(n)], 1)
        return dot(kron_own[...], own) + dot(kron_sib[...], other)

    def e_step(q, n):
        e = contract_p(q, n)
        free = iota((192, 128), 1) >= LANES
        for k in range(n):
            at = (q + k) % RIDERS * FREE
            rider = pltpu.roll(e_special[(q + k) // RIDERS], LANES - at, 1)
            row = jnp.where(free, rider, e[:, k * 128:(k + 1) * 128])
            for yy in range(2):
                for zz in range(4):
                    r = (yy * 4 + zz) * OCC
                    e_buf[yy, zz, rows_of(q + k, 1), :] = row[r:r + OCC]

    def unpack(sp, first, end):
        lane = iota((8, 128), 1)
        for src in range(4):
            for ib in range(0, OCC, 8):
                dst = pl.ds((src * 32 + KEPT + sp) * OCC + ib, 8)
                acc = e_all[dst] if first else jnp.zeros((8, 128), F32)
                for k in range(first, end):
                    row = e_all[pl.ds((src * 32 + sp * RIDERS + k) * OCC + ib, 8)]
                    acc = jnp.where(lane // FREE == k, pltpu.roll(row, (k + 1) * FREE % 128, 1), acc)
                e_all[dst] = acc

    def v_group(g):
        lhs = virt_v[g]
        for i in range(0, OCC, 2):
            parts = []
            for k in range(2):
                e = jnp.concatenate(
                    [e_all[pl.ds((src * 32 + g * QGRP) * OCC + i + k, QGRP, stride=OCC), :] for src in range(4)], 0)
                hi = e.astype(BF16)
                rest = e - hi.astype(F32)
                mid = rest.astype(BF16)
                low = (rest - mid.astype(F32)).astype(BF16)
                parts.append(jnp.concatenate([hi, mid, low], 0))
            v = dot(lhs, jnp.concatenate(parts, 1))
            for k in range(2):
                out_ref[i + k] += v[:, k * 128:k * 128 + LANES]

    def finish(g):
        y_own(g).wait_recv()
        q, n = CHUNKS[g]
        rows = rows_of(q, n)
        e_all[rows_of(z * 32 + q, n)] = e_buf[y, z, rows] + y_in[z, rows]
        z_wait(n, zn_sem.at[g])
        z_wait(2 * n, zc_sem.at[g])
        if g == 1:
            unpack(0, 0, 15)
        if g == 2:
            unpack(1, 0, 9)
        if g == 3:
            unpack(1, 9, 15)
        v_group(g)

    def step(s, carry):
        def transform(q, n, t):
            a_copy(q, n, t).wait()

            @pl.when(t + AHEAD < STEPS)
            def _():
                a_copy(2 * (t + AHEAD) - 4, 2, t + AHEAD).start()
            slot = q % SLOTS
            half_step(lambda p, qq: a_buf[p, slot + qq], q, n)
            if isinstance(q, int):
                pl.semaphore_wait(barrier, 5)
            h_copy(q, n, hr_sem.at[t % H_RING]).start()

        when_step(s, 0, STEPS, 0, transform)

        @pl.when(s == 2)
        def _():
            a_copy_late.start()

        @pl.when(s == LATE)
        def _():
            a_copy_late.wait()
            half_step(lambda p, qq: a_late[p], 31, 1)
            h_copy(31, 1, hl_sem).start()

        def to_e(q, n, t):
            h_copy(q, n, hr_sem.at[t % H_RING]).wait_recv()
            if isinstance(q, int):
                e_special[0] = contract_p(30, 1)
            else:
                e_step(q, n)
                y_cross(q, n, t).start()

        when_step(s, 0, STEPS, 1, to_e)

        @pl.when(s == LATE + 1)
        def _():
            h_copy(31, 1, hl_sem).wait_recv()
            e_special[1] = contract_p(31, 1)

        for k in range(GROUPS):
            @pl.when(s == NEAR_AT[k])
            def _():
                y_near(k).start()

            @pl.when(s == OWN_AT[k])
            def _():
                y_own(k).start()

        def to_z(q, n, t):
            y_cross(q, n, t).wait_recv()
            add_send(far, q, n, zc_sem.at[q // QGRP])
            add_send(far_near, q, n, zc_sem.at[q // QGRP])

        when_step(s, 1, STEPS, CROSS_SUM - 1, to_z)

        for k in range(GROUPS):
            @pl.when(s == NEAR_SUM[k])
            def _():
                y_near(k).wait_recv()
                add_send(near, *CHUNKS[k], zn_sem.at[k])

        for g in range(GROUPS - 1):
            @pl.when(s == V_AT[g])
            def _():
                finish(g)
        return carry

    lax.fori_loop(0, END, step, 0)
    finish(GROUPS - 1)

    pltpu.make_async_remote_copy(
        src_ref=h_buf.at[1 - core], dst_ref=h_in, send_sem=hs_sem, recv_sem=hl_sem,
        device_id={"dev": sib}, device_id_type=MESH).wait_send()
    y_copy(0, 4, 0, KEPT, yo_sem.at[0]).wait_send()
    rows = pl.ds(0, 3 * KEPT * OCC)
    pltpu.make_async_remote_copy(
        src_ref=e_all.at[rows], dst_ref=e_all.at[rows], send_sem=zs_sem, recv_sem=zn_sem.at[0],
        device_id={"dev2": near}, device_id_type=MESH).wait_send()


def solution(mesh):
    def local_block(ao_blk, c_occ, c_virt):
        hbm = pl.BlockSpec(memory_space=pltpu.HBM)
        dma = pltpu.SemaphoreType.DMA
        return pl.pallas_call(
            kernel,
            out_shape=jax.ShapeDtypeStruct((OCC, VIRT, LANES), F32),
            in_specs=[hbm, hbm, hbm],
            out_specs=pl.BlockSpec(memory_space=pltpu.VMEM),
            scratch_shapes=[
                pltpu.VMEM((32, SLOTS, 128, 128), BF16),
                pltpu.VMEM((32, 128, 128), BF16),
                pltpu.VMEM((2 * OCC, 256), BF16),
                pltpu.VMEM((256, 384), BF16),
                pltpu.VMEM((192, 256), BF16),
                pltpu.VMEM((192, 256), BF16),
                pltpu.VMEM((GROUPS, VIRT, 96), BF16),
                pltpu.VMEM((2, 32, 256, 128), BF16),
                pltpu.VMEM((32, 256, 128), BF16),
                pltpu.VMEM((SPECIAL, 192, 128), F32),
                pltpu.VMEM((2, 4, PART, 128), F32),
                pltpu.VMEM((4, PART, 128), F32),
                pltpu.VMEM((4 * PART, 128), F32),
                pltpu.VMEM((OCC, 128), BF16),
                pltpu.VMEM((VIRT, 128), BF16),
                dma((2,)), dma((8,)), dma,
                dma, dma((H_RING,)), dma,
                dma, dma((Y_RING,)), dma((GROUPS,)), dma((GROUPS,)),
                dma, dma((GROUPS,)), dma((GROUPS,)),
            ],
            compiler_params=pltpu.CompilerParams(
                collective_id=0, has_side_effects=True, vmem_limit_bytes=37 * 1024 * 1024),
        )(ao_blk, *(pltpu.with_memory_space_constraint(c.T, pltpu.HBM) for c in (c_occ, c_virt)))

    return jax.shard_map(
        local_block, mesh=mesh,
        in_specs=(P(("frag", "dev"), "dev2", None, None), P("frag", None), P("frag", None)),
        out_specs=P("frag", None, ("dev2", "dev")),
        check_vma=False)
```

```python
import functools

import jax
import jax.numpy as jnp
from jax import lax
from jax.experimental import pallas as pl
from jax.experimental.pallas import tpu as pltpu
from jax.sharding import PartitionSpec as P

MESH = pl.DeviceIdType.MESH
F32 = jnp.float32
BF16 = jnp.bfloat16
OCC = 24
VIRT = 80
LANES = 120
SPECIAL = 2
KEPT = 32 - SPECIAL
RIDERS = KEPT // SPECIAL
FREE = 128 - LANES
PART = 32 * OCC
STEPS = 17
LATE = 9
SLOTS = 16
AHEAD = 6
QGRP = 8
GROUPS = 4
H_RING = 4
Y_RING = 8
OWN = ((0, 8), (8, 8), (16, 8), (24, 6))
NEAR = ((0, 4), (4, 4), (8, 8), (16, 8), (24, 6))
SWITCH = 4
CROSS_SUM = 3
CROSS_SUM_2 = 4
NEAR_AT = (7, 8, 11, 15, 17)
NEAR_SUM = (11, 12, 15, 19, 21)
OWN_AT = (17, 17, 18, 19)
V_AT = (21, 22, 23)
END = 24


def dot(a, b):
    return jnp.dot(a, b, preferred_element_type=F32)


def dot_nt(a, b):
    return lax.dot_general(a, b, (((1,), (1,)), ((), ())), preferred_element_type=F32)


def iota(shape, dim):
    return lax.broadcasted_iota(jnp.int32, shape, dim)


def select(mask):
    return jnp.where(mask, 1.0, 0.0).astype(BF16)


def kernel(ao_ref, occ_hbm, virt_hbm, out_ref,
           a_buf, a_late, occ_lhs, virt_rhs, kron_own, kron_sib, virt_v,
           h_buf, h_in, e_special, e_buf, y_in, e_all, occ_ref, virt_ref,
           c_sem, a_sem, al_sem, hs_sem, hr_sem, hl_sem, ys_sem, yc_sem, yn_sem, yo_sem,
           zs_sem, zc_sem, zn_sem):
    z = lax.axis_index("dev2")
    dev = lax.axis_index("dev")
    y = dev // 2
    core = dev % 2
    sib = y * 2 + (1 - core)
    across = (1 - y) * 2 + core
    half = z // 2
    far = 3 * (1 - half)
    far_near = 2 - half
    near = 1 - z + 4 * half

    def rows_of(q, n):
        if not isinstance(q, int):
            q = pl.multiple_of(q * OCC, 8)
        else:
            q = q * OCC
        return pl.ds(q, n * OCC)

    def a_copy(q, n, s):
        return pltpu.make_async_copy(
            ao_ref.at[:, pl.ds(q, n)], a_buf.at[:, pl.ds(q % SLOTS, n)], a_sem.at[s % 8])

    a_copy_late = pltpu.make_async_copy(ao_ref.at[:, 31], a_late, al_sem)

    def h_copy(q, n, sem):
        return pltpu.make_async_remote_copy(
            src_ref=h_buf.at[1 - core, pl.ds(q, n)], dst_ref=h_in.at[pl.ds(q, n)],
            send_sem=hs_sem, recv_sem=sem,
            device_id={"dev": sib}, device_id_type=MESH)

    def y_copy(z0, zn, q, n, sem):
        return pltpu.make_async_remote_copy(
            src_ref=e_buf.at[1 - y, pl.ds(z0, zn), rows_of(q, n)],
            dst_ref=y_in.at[pl.ds(z0, zn), rows_of(q, n)],
            send_sem=ys_sem, recv_sem=sem,
            device_id={"dev": across}, device_id_type=MESH)

    def y_cross(q, n, s):
        return y_copy(2 * (1 - half), 2, q, n, yc_sem.at[s % Y_RING])

    def y_near(k):
        return y_copy(near, 1, *NEAR[k], yn_sem.at[k])

    def y_own(k):
        return y_copy(z, 1, *OWN[k], yo_sem.at[k])

    def add_send(zz, q, n, sem):
        rows = rows_of(q, n)
        e_buf[y, zz, rows] = e_buf[y, zz, rows] + y_in[zz, rows]
        pltpu.make_async_remote_copy(
            src_ref=e_buf.at[y, zz, rows], dst_ref=e_all.at[rows_of(z * 32 + q, n)],
            send_sem=zs_sem, recv_sem=sem,
            device_id={"dev2": zz}, device_id_type=MESH).start()

    def z_wait(n, sem):
        rows = pl.ds(0, n * OCC)
        pltpu.make_async_remote_copy(
            src_ref=e_all.at[rows], dst_ref=e_all.at[rows], send_sem=zs_sem, recv_sem=sem,
            device_id={"dev2": near}, device_id_type=MESH).wait_recv()

    def when_step(s, first, end, shift, do):
        t = s - shift

        if first == 0:
            @pl.when(t == 0)
            def _():
                do(30, 1, 0)

        if first < 3:
            @pl.when((t == 1) | (t == 2))
            def _():
                do(t - 1, 1, t)

        @pl.when((t >= max(first, 3)) & (t < end))
        def _():
            do(2 * t - 4, 2, t)

    barrier = pltpu.get_barrier_semaphore()
    for peer in ({"dev": sib}, {"dev": across}, {"dev2": (z + 1) % 4}, {"dev2": (z + 2) % 4}, {"dev2": (z + 3) % 4}):
        pl.semaphore_signal(barrier, inc=1, device_id=peer, device_id_type=MESH)

    c_copies = (pltpu.make_async_copy(occ_hbm, occ_ref, c_sem.at[0]),
                pltpu.make_async_copy(virt_hbm, virt_ref, c_sem.at[1]))
    for c in c_copies:
        c.start()
    a_copy(30, 1, 0).start()
    for i in range(OCC):
        out_ref[i] = jnp.zeros((VIRT, LANES), F32)
    for c in c_copies:
        c.wait()
    for s in range(1, AHEAD):
        a_copy(*((s - 1, 1) if s < 3 else (2 * s - 4, 2)), s).start()

    row = iota((OCC, OCC), 0)
    perm = select(iota((OCC, OCC), 1) == 3 * (row % 8) + row // 8)
    occ_t = dot(perm, occ_ref[...]).astype(BF16)
    zero = jnp.zeros((OCC, 128), BF16)
    occ_lhs[...] = jnp.concatenate(
        [jnp.concatenate([occ_t, zero], 1), jnp.concatenate([zero, occ_t], 1)], 0)
    row = iota((256, VIRT), 0)
    lane = row % 128
    pair = (row // 128) * LANES + lane
    for jj in range(3):
        pick = select((pair == jj * VIRT + iota((256, VIRT), 1)) & (lane < LANES))
        virt_rhs[pl.ds(jj * 128, 128), :] = lax.dot_general(virt_ref[...], pick, (((0,), (1,)), ((), ())), preferred_element_type=F32).astype(BF16)
    row = iota((192, OCC), 0)
    pick_i = select(row % OCC == iota((192, OCC), 1))
    occ_i = dot(pick_i, occ_ref[...]).astype(BF16)
    row = iota((192, 256), 0)
    keep = iota((192, 256), 1) % 8 == 2 * ((row % 96) // OCC) + row // 96
    for dst, who in ((kron_own, dev), (kron_sib, sib)):
        pick_p = select(iota((128, 256), 1) // 8 + who * 32 == iota((128, 256), 0))
        dst[...] = jnp.where(keep, dot(occ_i, pick_p), 0.0).astype(BF16)
    col = iota((128, 96), 1)
    for g in range(GROUPS):
        pick_q = select(iota((128, 96), 0) == (col % 32) // QGRP * 32 + g * QGRP + col % QGRP)
        virt_v[g] = dot(virt_ref[...], pick_q).astype(BF16)

    def half_step(tiles, q, n):
        rows = []
        for qq in range(n):
            for p in range(0, 32, 4):
                a = [tiles(p + k, qq) for k in range(4)]
                w = jnp.concatenate(
                    [jnp.concatenate(a[:2], 1), jnp.concatenate(a[2:], 1)], 0)
                r = dot(occ_lhs[...], w)
                for k in range(4):
                    part = r[(k // 2) * OCC:(k // 2 + 1) * OCC, (k % 2) * 128:(k % 2 + 1) * 128]
                    rows.append(jnp.concatenate([part[0:8], part[8:16], part[16:24]], 1))
        t_one = jnp.concatenate(rows, 0).astype(BF16)
        h = dot(t_one, virt_rhs[...]).astype(BF16)
        for qq in range(n):
            h_buf[0, q + qq] = h[qq * 256:(qq + 1) * 256, :128]
            h_buf[1, q + qq] = h[qq * 256:(qq + 1) * 256, 128:]

    def contract_p(q, n):
        own = jnp.concatenate([h_buf[core, q + k] for k in range(n)], 1)
        other = jnp.concatenate([h_in[q + k] for k in range(n)], 1)
        return dot(kron_own[...], own) + dot(kron_sib[...], other)

    def e_step(q, n):
        e = contract_p(q, n)
        free = iota((192, 128), 1) >= LANES
        for k in range(n):
            at = (q + k) % RIDERS * FREE
            rider = pltpu.roll(e_special[(q + k) // RIDERS], LANES - at, 1)
            row = jnp.where(free, rider, e[:, k * 128:(k + 1) * 128])
            for yy in range(2):
                for zz in range(4):
                    r = (yy * 4 + zz) * OCC
                    e_buf[yy, zz, rows_of(q + k, 1), :] = row[r:r + OCC]

    def unpack(sp, first, end):
        lane = iota((8, 128), 1)
        for src in range(4):
            for ib in range(0, OCC, 8):
                dst = pl.ds((src * 32 + KEPT + sp) * OCC + ib, 8)
                acc = e_all[dst] if first else jnp.zeros((8, 128), F32)
                for k in range(first, end):
                    row = e_all[pl.ds((src * 32 + sp * RIDERS + k) * OCC + ib, 8)]
                    acc = jnp.where(lane // FREE == k, pltpu.roll(row, (k + 1) * FREE % 128, 1), acc)
                e_all[dst] = acc

    def v_group(g):
        lhs = virt_v[g]
        for i in range(0, OCC, 2):
            parts = []
            for k in range(2):
                e = jnp.concatenate(
                    [e_all[pl.ds((src * 32 + g * QGRP) * OCC + i + k, QGRP, stride=OCC), :] for src in range(4)], 0)
                hi = e.astype(BF16)
                rest = e - hi.astype(F32)
                mid = rest.astype(BF16)
                low = (rest - mid.astype(F32)).astype(BF16)
                parts.append(jnp.concatenate([hi, mid, low], 0))
            v = dot(lhs, jnp.concatenate(parts, 1))
            for k in range(2):
                out_ref[i + k] += v[:, k * 128:k * 128 + LANES]

    def finish(g):
        y_own(g).wait_recv()
        q, n = OWN[g]
        rows = rows_of(q, n)
        e_all[rows_of(z * 32 + q, n)] = e_buf[y, z, rows] + y_in[z, rows]
        z_wait(n, zn_sem.at[g])
        z_wait(2 * n, zc_sem.at[g])
        if g == 1:
            unpack(0, 0, 15)
        if g == 2:
            unpack(1, 0, 9)
        if g == 3:
            unpack(1, 9, 15)
        v_group(g)

    def step(s, carry):
        def transform(q, n, t):
            a_copy(q, n, t).wait()

            @pl.when(t + AHEAD < STEPS)
            def _():
                a_copy(2 * (t + AHEAD) - 4, 2, t + AHEAD).start()
            slot = q % SLOTS
            half_step(lambda p, qq: a_buf[p, slot + qq], q, n)
            if isinstance(q, int):
                pl.semaphore_wait(barrier, 5)
            h_copy(q, n, hr_sem.at[t % H_RING]).start()

        when_step(s, 0, STEPS, 0, transform)

        @pl.when(s == 2)
        def _():
            a_copy_late.start()

        @pl.when(s == LATE)
        def _():
            a_copy_late.wait()
            half_step(lambda p, qq: a_late[p], 31, 1)
            h_copy(31, 1, hl_sem).start()

        @pl.when(s == LATE + 1)
        def _():
            h_copy(31, 1, hl_sem).wait_recv()
            e_special[1] = contract_p(31, 1)

        def to_e(q, n, t):
            h_copy(q, n, hr_sem.at[t % H_RING]).wait_recv()
            if isinstance(q, int):
                e_special[0] = contract_p(30, 1)
            else:
                e_step(q, n)
                y_cross(q, n, t).start()

        when_step(s, 0, STEPS, 1, to_e)

        for k in range(len(NEAR)):
            @pl.when(s == NEAR_AT[k])
            def _():
                y_near(k).start()

        for k in range(GROUPS):
            @pl.when(s == OWN_AT[k])
            def _():
                y_own(k).start()

        def to_z(q, n, t):
            y_cross(q, n, t).wait_recv()
            add_send(far, q, n, zc_sem.at[q // QGRP])
            add_send(far_near, q, n, zc_sem.at[q // QGRP])

        when_step(s, 1, SWITCH, CROSS_SUM, to_z)
        when_step(s, SWITCH, STEPS, CROSS_SUM_2, to_z)

        for k in range(len(NEAR)):
            @pl.when(s == NEAR_SUM[k])
            def _():
                y_near(k).wait_recv()
                add_send(near, *NEAR[k], zn_sem.at[NEAR[k][0] // QGRP])

        for g in range(GROUPS - 1):
            @pl.when(s == V_AT[g])
            def _():
                finish(g)
        return carry

    lax.fori_loop(0, END, step, 0)
    finish(GROUPS - 1)

    pltpu.make_async_remote_copy(
        src_ref=h_buf.at[1 - core], dst_ref=h_in, send_sem=hs_sem, recv_sem=hl_sem,
        device_id={"dev": sib}, device_id_type=MESH).wait_send()
    y_copy(0, 4, 0, KEPT, yo_sem.at[0]).wait_send()
    rows = pl.ds(0, 3 * KEPT * OCC)
    pltpu.make_async_remote_copy(
        src_ref=e_all.at[rows], dst_ref=e_all.at[rows], send_sem=zs_sem, recv_sem=zn_sem.at[0],
        device_id={"dev2": near}, device_id_type=MESH).wait_send()


def solution(mesh):
    def local_block(ao_blk, c_occ, c_virt):
        hbm = pl.BlockSpec(memory_space=pltpu.HBM)
        dma = pltpu.SemaphoreType.DMA
        return pl.pallas_call(
            kernel,
            out_shape=jax.ShapeDtypeStruct((OCC, VIRT, LANES), F32),
            in_specs=[hbm, hbm, hbm],
            out_specs=pl.BlockSpec(memory_space=pltpu.VMEM),
            scratch_shapes=[
                pltpu.VMEM((32, SLOTS, 128, 128), BF16),
                pltpu.VMEM((32, 128, 128), BF16),
                pltpu.VMEM((2 * OCC, 256), BF16),
                pltpu.VMEM((384, 256), BF16),
                pltpu.VMEM((192, 256), BF16),
                pltpu.VMEM((192, 256), BF16),
                pltpu.VMEM((GROUPS, VIRT, 96), BF16),
                pltpu.VMEM((2, 32, 256, 128), BF16),
                pltpu.VMEM((32, 256, 128), BF16),
                pltpu.VMEM((SPECIAL, 192, 128), F32),
                pltpu.VMEM((2, 4, PART, 128), F32),
                pltpu.VMEM((4, PART, 128), F32),
                pltpu.VMEM((4 * PART, 128), F32),
                pltpu.VMEM((OCC, 128), BF16),
                pltpu.VMEM((VIRT, 128), BF16),
                dma((2,)), dma((8,)), dma,
                dma, dma((H_RING,)), dma,
                dma, dma((Y_RING,)), dma((len(NEAR),)), dma((GROUPS,)),
                dma, dma((GROUPS,)), dma((GROUPS,)),
            ],
            compiler_params=pltpu.CompilerParams(
                collective_id=0, has_side_effects=True, vmem_limit_bytes=37 * 1024 * 1024),
        )(ao_blk, *(pltpu.with_memory_space_constraint(c.T, pltpu.HBM) for c in (c_occ, c_virt)))

    return jax.shard_map(
        local_block, mesh=mesh,
        in_specs=(P(("frag", "dev"), "dev2", None, None), P("frag", None), P("frag", None)),
        out_specs=P("frag", None, ("dev2", "dev")),
        check_vma=False)
```

```python
import functools

import jax
import jax.numpy as jnp
from jax import lax
from jax.experimental import pallas as pl
from jax.experimental.pallas import tpu as pltpu
from jax.sharding import PartitionSpec as P

MESH = pl.DeviceIdType.MESH
F32 = jnp.float32
BF16 = jnp.bfloat16
OCC = 24
VIRT = 80
LANES = 120
SPECIAL = 2
KEPT = 32 - SPECIAL
RIDERS = KEPT // SPECIAL
FREE = 128 - LANES
PART = 32 * OCC
STEPS = 16
HALF = 8
SLOTS = 8
AHEAD = 6
QGRP = 8
GROUPS = 4
H_RING = 4
Y_RING = 8
OWN = ((0, 8), (8, 8), (16, 8), (24, 6))
NEAR = ((0, 4), (4, 4), (8, 8), (16, 8), (24, 6))
SWITCH = 3
CROSS_SUM = 3
CROSS_SUM_2 = 4
NEAR_AT = (10, 12, 13, 15, 16)
NEAR_SUM = (14, 14, 17, 19, 20)
OWN_AT = (16, 16, 17, 18)
V_AT = (20, 21, 22)
END = 23
CROSS_Q = (7, 9, 8, 6)


def dot(a, b):
    return jnp.dot(a, b, preferred_element_type=F32)


def dot_nt(a, b):
    return lax.dot_general(a, b, (((1,), (1,)), ((), ())), preferred_element_type=F32)


def iota(shape, dim):
    return lax.broadcasted_iota(jnp.int32, shape, dim)


def select(mask):
    return jnp.where(mask, 1.0, 0.0).astype(BF16)


def kernel(ao_ref, occ_hbm, virt_hbm, out_ref,
           a_buf, occ_lhs, virt_rhs, kron_own, kron_sib, virt_v,
           h_buf, h_in, e_special, e_buf, y_in, e_all, occ_ref, virt_ref,
           c_sem, a_sem, hs_sem, hr_sem, ys_sem, yc_sem, yn_sem, yo_sem,
           zs_sem, zc_sem, zn_sem):
    z = lax.axis_index("dev2")
    dev = lax.axis_index("dev")
    y = dev // 2
    core = dev % 2
    sib = y * 2 + (1 - core)
    across = (1 - y) * 2 + core
    half = z // 2
    far = 3 * (1 - half)
    far_near = 2 - half
    near = 1 - z + 4 * half

    def rows_of(q, n):
        if not isinstance(q, int):
            q = pl.multiple_of(q * OCC, 8)
        else:
            q = q * OCC
        return pl.ds(q, n * OCC)

    def first_q(s):
        if isinstance(s, int):
            return s // HALF * RIDERS + max(2 * (s % HALF) - 1, 0)
        return s // HALF * RIDERS + jnp.maximum(2 * (s % HALF) - 1, 0)

    def a_start(s):
        special = s % HALF == 0
        q = first_q(s)
        for k in range(2):
            if isinstance(s, int):
                at = (KEPT + s // HALF if k == 0 else q) if special else q + k
            else:
                at = jnp.where(special, (q, KEPT + s // HALF)[1 - k], q + k)
            pltpu.make_async_copy(ao_ref.at[:, at], a_buf.at[s % SLOTS, :, k], a_sem.at[s % SLOTS]).start()

    def a_wait(s):
        pltpu.make_async_copy(ao_ref.at[:, pl.ds(0, 2)], a_buf.at[s % SLOTS], a_sem.at[s % SLOTS]).wait()

    def h_copy(s):
        rows = pl.ds(s * 2, 2)
        return pltpu.make_async_remote_copy(
            src_ref=h_buf.at[1 - core, rows], dst_ref=h_in.at[rows],
            send_sem=hs_sem, recv_sem=hr_sem.at[s % H_RING],
            device_id={"dev": sib}, device_id_type=MESH)

    def y_copy(z0, zn, q, n, sem):
        return pltpu.make_async_remote_copy(
            src_ref=e_buf.at[1 - y, pl.ds(z0, zn), rows_of(q, n)],
            dst_ref=y_in.at[pl.ds(z0, zn), rows_of(q, n)],
            send_sem=ys_sem, recv_sem=sem,
            device_id={"dev": across}, device_id_type=MESH)

    def y_cross(q, n, s):
        return y_copy(2 * (1 - half), 2, q, n, yc_sem.at[s % Y_RING])

    def y_near(k):
        return y_copy(near, 1, *NEAR[k], yn_sem.at[k])

    def y_own(k):
        return y_copy(z, 1, *OWN[k], yo_sem.at[k])

    def add_send(zz, q, n, sem):
        rows = rows_of(q, n)
        e_buf[y, zz, rows] = e_buf[y, zz, rows] + y_in[zz, rows]
        pltpu.make_async_remote_copy(
            src_ref=e_buf.at[y, zz, rows], dst_ref=e_all.at[rows_of(z * 32 + q, n)],
            send_sem=zs_sem, recv_sem=sem,
            device_id={"dev2": zz}, device_id_type=MESH).start()

    def z_wait(n, sem):
        rows = pl.ds(0, n * OCC)
        pltpu.make_async_remote_copy(
            src_ref=e_all.at[rows], dst_ref=e_all.at[rows], send_sem=zs_sem, recv_sem=sem,
            device_id={"dev2": near}, device_id_type=MESH).wait_recv()

    def when_step(s, first, end, shift, do):
        t = s - shift

        @pl.when((t >= first) & (t < end) & (t % HALF == 0))
        def _():
            do(t // HALF * RIDERS, 1, t)

        @pl.when((t >= first) & (t < end) & (t % HALF != 0))
        def _():
            do(first_q(t), 2, t)

    barrier = pltpu.get_barrier_semaphore()
    for peer in ({"dev": sib}, {"dev": across}, {"dev2": (z + 1) % 4}, {"dev2": (z + 2) % 4}, {"dev2": (z + 3) % 4}):
        pl.semaphore_signal(barrier, inc=1, device_id=peer, device_id_type=MESH)

    c_copies = (pltpu.make_async_copy(occ_hbm, occ_ref, c_sem.at[0]),
                pltpu.make_async_copy(virt_hbm, virt_ref, c_sem.at[1]))
    for c in c_copies:
        c.start()
    a_start(0)
    for i in range(OCC):
        out_ref[i] = jnp.zeros((VIRT, LANES), F32)
    for c in c_copies:
        c.wait()
    for s in range(1, AHEAD):
        a_start(s)

    row = iota((OCC, OCC), 0)
    perm = select(iota((OCC, OCC), 1) == 3 * (row % 8) + row // 8)
    occ_t = dot(perm, occ_ref[...]).astype(BF16)
    zero = jnp.zeros((OCC, 128), BF16)
    occ_lhs[...] = jnp.concatenate(
        [jnp.concatenate([occ_t, zero], 1), jnp.concatenate([zero, occ_t], 1)], 0)
    row = iota((256, VIRT), 0)
    lane = row % 128
    pair = (row // 128) * LANES + lane
    for jj in range(3):
        pick = select((pair == jj * VIRT + iota((256, VIRT), 1)) & (lane < LANES))
        virt_rhs[pl.ds(jj * 128, 128), :] = lax.dot_general(virt_ref[...], pick, (((0,), (1,)), ((), ())), preferred_element_type=F32).astype(BF16)
    row = iota((192, OCC), 0)
    pick_i = select(row % OCC == iota((192, OCC), 1))
    occ_i = dot(pick_i, occ_ref[...]).astype(BF16)
    row = iota((192, 256), 0)
    keep = iota((192, 256), 1) % 8 == 2 * ((row % 96) // OCC) + row // 96
    for dst, who in ((kron_own, dev), (kron_sib, sib)):
        pick_p = select(iota((128, 256), 1) // 8 + who * 32 == iota((128, 256), 0))
        dst[...] = jnp.where(keep, dot(occ_i, pick_p), 0.0).astype(BF16)
    col = iota((128, 96), 1)
    for g in range(GROUPS):
        pick_q = select(iota((128, 96), 0) == (col % 32) // QGRP * 32 + g * QGRP + col % QGRP)
        virt_v[g] = dot(virt_ref[...], pick_q).astype(BF16)

    def half_step(s):
        rows = []
        for qq in range(2):
            for p in range(0, 32, 4):
                a = [a_buf[s % SLOTS, p + k, qq] for k in range(4)]
                w = jnp.concatenate(
                    [jnp.concatenate(a[:2], 1), jnp.concatenate(a[2:], 1)], 0)
                r = dot(occ_lhs[...], w)
                for k in range(4):
                    part = r[(k // 2) * OCC:(k // 2 + 1) * OCC, (k % 2) * 128:(k % 2 + 1) * 128]
                    rows.append(jnp.concatenate([part[0:8], part[8:16], part[16:24]], 1))
        t_one = jnp.concatenate(rows, 0).astype(BF16)
        h = dot(t_one, virt_rhs[...]).astype(BF16)
        for qq in range(2):
            h_buf[0, s * 2 + qq] = h[qq * 256:(qq + 1) * 256, :128]
            h_buf[1, s * 2 + qq] = h[qq * 256:(qq + 1) * 256, 128:]

    def contract_p(s):
        own = jnp.concatenate([h_buf[core, s * 2 + k] for k in range(2)], 1)
        other = jnp.concatenate([h_in[s * 2 + k] for k in range(2)], 1)
        return dot(kron_own[...], own) + dot(kron_sib[...], other)

    def e_step(q, n, s):
        e = contract_p(s)
        free = iota((192, 128), 1) >= LANES
        g = s // HALF
        if n == 1:
            e_special[g] = e[:, :128]
        for k in range(n):
            if n == 1:
                rider = pltpu.roll(e[:, :128], LANES, 1)
            else:
                rider = pltpu.roll(e_special[g], LANES - (q + k) % RIDERS * FREE, 1)
            k_at = k + 2 - n
            row = jnp.where(free, rider, e[:, k_at * 128:(k_at + 1) * 128])
            for yy in range(2):
                for zz in range(4):
                    r = (yy * 4 + zz) * OCC
                    e_buf[yy, zz, rows_of(q + k, 1), :] = row[r:r + OCC]

    def unpack(sp, first, end):
        lane = iota((8, 128), 1)
        for src in range(4):
            for ib in range(0, OCC, 8):
                dst = pl.ds((src * 32 + KEPT + sp) * OCC + ib, 8)
                acc = e_all[dst] if first else jnp.zeros((8, 128), F32)
                for k in range(first, end):
                    row = e_all[pl.ds((src * 32 + sp * RIDERS + k) * OCC + ib, 8)]
                    acc = jnp.where(lane // FREE == k, pltpu.roll(row, (k + 1) * FREE % 128, 1), acc)
                e_all[dst] = acc

    def v_group(g):
        lhs = virt_v[g]
        for i in range(0, OCC, 2):
            parts = []
            for k in range(2):
                e = jnp.concatenate(
                    [e_all[pl.ds((src * 32 + g * QGRP) * OCC + i + k, QGRP, stride=OCC), :] for src in range(4)], 0)
                hi = e.astype(BF16)
                rest = e - hi.astype(F32)
                mid = rest.astype(BF16)
                low = (rest - mid.astype(F32)).astype(BF16)
                parts.append(jnp.concatenate([hi, mid, low], 0))
            v = dot(lhs, jnp.concatenate(parts, 1))
            for k in range(2):
                out_ref[i + k] += v[:, k * 128:k * 128 + LANES]

    def finish(g):
        y_own(g).wait_recv()
        q, n = OWN[g]
        rows = rows_of(q, n)
        e_all[rows_of(z * 32 + q, n)] = e_buf[y, z, rows] + y_in[z, rows]
        z_wait(n, zn_sem.at[g])
        for k in ((0, 1), (), (2,), (3,))[g]:
            z_wait(2 * CROSS_Q[k], zc_sem.at[k])
        if g == 1:
            unpack(0, 0, 15)
        if g == 2:
            unpack(1, 0, 9)
        if g == 3:
            unpack(1, 9, 15)
        v_group(g)

    def step(s, carry):
        @pl.when(s < STEPS)
        def _():
            a_wait(s)

            @pl.when(s + AHEAD < STEPS)
            def _():
                a_start(s + AHEAD)
            half_step(s)

            @pl.when(s == 0)
            def _():
                pl.semaphore_wait(barrier, 5)
            h_copy(s).start()

        def to_e(q, n, t):
            h_copy(t).wait_recv()
            e_step(q, n, t)
            y_cross(q, n, t).start()

        when_step(s, 0, STEPS, 1, to_e)

        for k in range(len(NEAR)):
            @pl.when(s == NEAR_AT[k])
            def _():
                y_near(k).start()

        for k in range(GROUPS):
            @pl.when(s == OWN_AT[k])
            def _():
                y_own(k).start()

        def to_z(q, n, t):
            y_cross(q, n, t).wait_recv()
            add_send(far, q, n, zc_sem.at[(q + n - 1) // QGRP])
            add_send(far_near, q, n, zc_sem.at[(q + n - 1) // QGRP])

        when_step(s, 0, SWITCH, CROSS_SUM, to_z)
        when_step(s, SWITCH, STEPS, CROSS_SUM_2, to_z)

        for k in range(len(NEAR)):
            @pl.when(s == NEAR_SUM[k])
            def _():
                y_near(k).wait_recv()
                add_send(near, *NEAR[k], zn_sem.at[NEAR[k][0] // QGRP])

        for g in range(GROUPS - 1):
            @pl.when(s == V_AT[g])
            def _():
                finish(g)
        return carry

    lax.fori_loop(0, END, step, 0)
    finish(GROUPS - 1)

    pltpu.make_async_remote_copy(
        src_ref=h_buf.at[1 - core], dst_ref=h_in, send_sem=hs_sem, recv_sem=hr_sem.at[0],
        device_id={"dev": sib}, device_id_type=MESH).wait_send()
    y_copy(0, 4, 0, KEPT, yo_sem.at[0]).wait_send()
    rows = pl.ds(0, 3 * KEPT * OCC)
    pltpu.make_async_remote_copy(
        src_ref=e_all.at[rows], dst_ref=e_all.at[rows], send_sem=zs_sem, recv_sem=zn_sem.at[0],
        device_id={"dev2": near}, device_id_type=MESH).wait_send()


def solution(mesh):
    def local_block(ao_blk, c_occ, c_virt):
        hbm = pl.BlockSpec(memory_space=pltpu.HBM)
        dma = pltpu.SemaphoreType.DMA
        return pl.pallas_call(
            kernel,
            out_shape=jax.ShapeDtypeStruct((OCC, VIRT, LANES), F32),
            in_specs=[hbm, hbm, hbm],
            out_specs=pl.BlockSpec(memory_space=pltpu.VMEM),
            scratch_shapes=[
                pltpu.VMEM((SLOTS, 32, 2, 128, 128), BF16),
                pltpu.VMEM((2 * OCC, 256), BF16),
                pltpu.VMEM((384, 256), BF16),
                pltpu.VMEM((192, 256), BF16),
                pltpu.VMEM((192, 256), BF16),
                pltpu.VMEM((GROUPS, VIRT, 96), BF16),
                pltpu.VMEM((2, 32, 256, 128), BF16),
                pltpu.VMEM((32, 256, 128), BF16),
                pltpu.VMEM((SPECIAL, 192, 128), F32),
                pltpu.VMEM((2, 4, PART, 128), F32),
                pltpu.VMEM((4, PART, 128), F32),
                pltpu.VMEM((4 * PART, 128), F32),
                pltpu.VMEM((OCC, 128), BF16),
                pltpu.VMEM((VIRT, 128), BF16),
                dma((2,)), dma((SLOTS,)),
                dma, dma((H_RING,)),
                dma, dma((Y_RING,)), dma((len(NEAR),)), dma((GROUPS,)),
                dma, dma((GROUPS,)), dma((GROUPS,)),
            ],
            compiler_params=pltpu.CompilerParams(
                collective_id=0, has_side_effects=True, vmem_limit_bytes=37 * 1024 * 1024),
        )(ao_blk, *(pltpu.with_memory_space_constraint(c.T, pltpu.HBM) for c in (c_occ, c_virt)))

    return jax.shard_map(
        local_block, mesh=mesh,
        in_specs=(P(("frag", "dev"), "dev2", None, None), P("frag", None), P("frag", None)),
        out_specs=P("frag", None, ("dev2", "dev")),
        check_vma=False)
```

```python
import functools

import jax
import jax.numpy as jnp
from jax import lax
from jax.experimental import pallas as pl
from jax.experimental.pallas import tpu as pltpu
from jax.sharding import PartitionSpec as P

MESH = pl.DeviceIdType.MESH
F32 = jnp.float32
BF16 = jnp.bfloat16
OCC = 24
VIRT = 80
LANES = 120
SPECIAL = 2
KEPT = 32 - SPECIAL
RIDERS = KEPT // SPECIAL
FREE = 128 - LANES
PART = 32 * OCC
STEPS = 16
HALF = 8
SLOTS = 8
AHEAD = 6
QGRP = 8
GROUPS = 4
H_RING = 4
Y_RING = 8
OWN = ((0, 8), (8, 8), (16, 8), (24, 6))
NEAR = ((0, 8), (8, 8), (16, 8), (24, 6))
SWITCH = 3
CROSS_SUM = 3
CROSS_SUM_2 = 4
NEAR_AT = (11, 13, 15, 16)
NEAR_SUM = (14, 17, 19, 20)
OWN_AT = (16, 16, 17, 18)
V_AT = (20, 21, 22)
END = 23
CROSS_Q = (7, 9, 8, 6)


def dot(a, b):
    return jnp.dot(a, b, preferred_element_type=F32)


def dot_nt(a, b):
    return lax.dot_general(a, b, (((1,), (1,)), ((), ())), preferred_element_type=F32)


def iota(shape, dim):
    return lax.broadcasted_iota(jnp.int32, shape, dim)


def select(mask):
    return jnp.where(mask, 1.0, 0.0).astype(BF16)


def kernel(ao_ref, occ_hbm, virt_hbm, out_ref,
           a_buf, occ_lhs, virt_rhs, kron_own, kron_sib, virt_v,
           h_buf, h_in, e_special, e_buf, y_in, e_all, occ_ref, virt_ref,
           c_sem, a_sem, hs_sem, hr_sem, ys_sem, yc_sem, yn_sem, yo_sem,
           zs_sem, zc_sem, zn_sem):
    z = lax.axis_index("dev2")
    dev = lax.axis_index("dev")
    y = dev // 2
    core = dev % 2
    sib = y * 2 + (1 - core)
    across = (1 - y) * 2 + core
    half = z // 2
    far = 3 * (1 - half)
    far_near = 2 - half
    near = 1 - z + 4 * half

    def rows_of(q, n):
        if not isinstance(q, int):
            q = pl.multiple_of(q * OCC, 8)
        else:
            q = q * OCC
        return pl.ds(q, n * OCC)

    def first_q(s):
        if isinstance(s, int):
            return s // HALF * RIDERS + max(2 * (s % HALF) - 1, 0)
        return s // HALF * RIDERS + jnp.maximum(2 * (s % HALF) - 1, 0)

    def a_start(s):
        special = s % HALF == 0
        q = first_q(s)
        for k in range(2):
            if isinstance(s, int):
                at = (KEPT + s // HALF if k == 0 else q) if special else q + k
            else:
                at = jnp.where(special, (q, KEPT + s // HALF)[1 - k], q + k)
            pltpu.make_async_copy(ao_ref.at[:, at], a_buf.at[s % SLOTS, :, k], a_sem.at[s % SLOTS]).start()

    def a_wait(s):
        pltpu.make_async_copy(ao_ref.at[:, pl.ds(0, 2)], a_buf.at[s % SLOTS], a_sem.at[s % SLOTS]).wait()

    def h_copy(s):
        rows = pl.ds(s * 2, 2)
        return pltpu.make_async_remote_copy(
            src_ref=h_buf.at[1 - core, rows], dst_ref=h_in.at[rows],
            send_sem=hs_sem, recv_sem=hr_sem.at[s % H_RING],
            device_id={"dev": sib}, device_id_type=MESH)

    def y_copy(z0, zn, q, n, sem):
        return pltpu.make_async_remote_copy(
            src_ref=e_buf.at[1 - y, pl.ds(z0, zn), rows_of(q, n)],
            dst_ref=y_in.at[pl.ds(z0, zn), rows_of(q, n)],
            send_sem=ys_sem, recv_sem=sem,
            device_id={"dev": across}, device_id_type=MESH)

    def y_cross(q, n, s):
        return y_copy(2 * (1 - half), 2, q, n, yc_sem.at[s % Y_RING])

    def y_near(k):
        return y_copy(near, 1, *NEAR[k], yn_sem.at[k])

    def y_own(k):
        return y_copy(z, 1, *OWN[k], yo_sem.at[k])

    def add_send(zz, q, n, sem):
        rows = rows_of(q, n)
        e_buf[y, zz, rows] = e_buf[y, zz, rows] + y_in[zz, rows]
        pltpu.make_async_remote_copy(
            src_ref=e_buf.at[y, zz, rows], dst_ref=e_all.at[rows_of(z * 32 + q, n)],
            send_sem=zs_sem, recv_sem=sem,
            device_id={"dev2": zz}, device_id_type=MESH).start()

    def z_wait(n, sem):
        rows = pl.ds(0, n * OCC)
        pltpu.make_async_remote_copy(
            src_ref=e_all.at[rows], dst_ref=e_all.at[rows], send_sem=zs_sem, recv_sem=sem,
            device_id={"dev2": near}, device_id_type=MESH).wait_recv()

    def when_step(s, first, end, shift, do):
        t = s - shift

        @pl.when((t >= first) & (t < end) & (t % HALF == 0))
        def _():
            do(t // HALF * RIDERS, 1, t)

        @pl.when((t >= first) & (t < end) & (t % HALF != 0))
        def _():
            do(first_q(t), 2, t)

    barrier = pltpu.get_barrier_semaphore()
    for peer in ({"dev": sib}, {"dev": across}, {"dev2": (z + 1) % 4}, {"dev2": (z + 2) % 4}, {"dev2": (z + 3) % 4}):
        pl.semaphore_signal(barrier, inc=1, device_id=peer, device_id_type=MESH)

    c_copies = (pltpu.make_async_copy(occ_hbm, occ_ref, c_sem.at[0]),
                pltpu.make_async_copy(virt_hbm, virt_ref, c_sem.at[1]))
    for c in c_copies:
        c.start()
    a_start(0)
    for i in range(OCC):
        out_ref[i] = jnp.zeros((VIRT, LANES), F32)
    for c in c_copies:
        c.wait()
    for s in range(1, AHEAD):
        a_start(s)

    row = iota((OCC, OCC), 0)
    perm = select(iota((OCC, OCC), 1) == 3 * (row % 8) + row // 8)
    occ_t = dot(perm, occ_ref[...]).astype(BF16)
    zero = jnp.zeros((OCC, 128), BF16)
    occ_lhs[...] = jnp.concatenate(
        [jnp.concatenate([occ_t, zero], 1), jnp.concatenate([zero, occ_t], 1)], 0)
    row = iota((256, VIRT), 0)
    lane = row % 128
    pair = (row // 128) * LANES + lane
    for jj in range(3):
        pick = select((pair == jj * VIRT + iota((256, VIRT), 1)) & (lane < LANES))
        virt_rhs[pl.ds(jj * 128, 128), :] = lax.dot_general(virt_ref[...], pick, (((0,), (1,)), ((), ())), preferred_element_type=F32).astype(BF16)
    row = iota((192, OCC), 0)
    pick_i = select(row % OCC == iota((192, OCC), 1))
    occ_i = dot(pick_i, occ_ref[...]).astype(BF16)
    row = iota((192, 256), 0)
    keep = iota((192, 256), 1) % 8 == 2 * ((row % 96) // OCC) + row // 96
    for dst, who in ((kron_own, dev), (kron_sib, sib)):
        pick_p = select(iota((128, 256), 1) // 8 + who * 32 == iota((128, 256), 0))
        dst[...] = jnp.where(keep, dot(occ_i, pick_p), 0.0).astype(BF16)
    col = iota((128, 96), 1)
    for g in range(GROUPS):
        pick_q = select(iota((128, 96), 0) == (col % 32) // QGRP * 32 + g * QGRP + col % QGRP)
        virt_v[g] = dot(virt_ref[...], pick_q).astype(BF16)

    def half_step(s):
        rows = []
        for qq in range(2):
            for p in range(0, 32, 4):
                a = [a_buf[s % SLOTS, p + k, qq] for k in range(4)]
                w = jnp.concatenate(
                    [jnp.concatenate(a[:2], 1), jnp.concatenate(a[2:], 1)], 0)
                r = dot(occ_lhs[...], w)
                for k in range(4):
                    part = r[(k // 2) * OCC:(k // 2 + 1) * OCC, (k % 2) * 128:(k % 2 + 1) * 128]
                    rows.append(jnp.concatenate([part[0:8], part[8:16], part[16:24]], 1))
        t_one = jnp.concatenate(rows, 0).astype(BF16)
        h = dot(t_one, virt_rhs[...]).astype(BF16)
        for qq in range(2):
            h_buf[0, s * 2 + qq] = h[qq * 256:(qq + 1) * 256, :128]
            h_buf[1, s * 2 + qq] = h[qq * 256:(qq + 1) * 256, 128:]

    def contract_p(s):
        own = jnp.concatenate([h_buf[core, s * 2 + k] for k in range(2)], 1)
        other = jnp.concatenate([h_in[s * 2 + k] for k in range(2)], 1)
        return dot(kron_own[...], own) + dot(kron_sib[...], other)

    def e_step(q, n, s):
        e = contract_p(s)
        free = iota((192, 128), 1) >= LANES
        g = s // HALF
        if n == 1:
            e_special[g] = e[:, :128]
        for k in range(n):
            if n == 1:
                rider = pltpu.roll(e[:, :128], LANES, 1)
            else:
                rider = pltpu.roll(e_special[g], LANES - (q + k) % RIDERS * FREE, 1)
            k_at = k + 2 - n
            row = jnp.where(free, rider, e[:, k_at * 128:(k_at + 1) * 128])
            for yy in range(2):
                for zz in range(4):
                    r = (yy * 4 + zz) * OCC
                    e_buf[yy, zz, rows_of(q + k, 1), :] = row[r:r + OCC]

    def unpack(sp, first, end):
        lane = iota((8, 128), 1)
        for src in range(4):
            for ib in range(0, OCC, 8):
                dst = pl.ds((src * 32 + KEPT + sp) * OCC + ib, 8)
                acc = e_all[dst] if first else jnp.zeros((8, 128), F32)
                for k in range(first, end):
                    row = e_all[pl.ds((src * 32 + sp * RIDERS + k) * OCC + ib, 8)]
                    acc = jnp.where(lane // FREE == k, pltpu.roll(row, (k + 1) * FREE % 128, 1), acc)
                e_all[dst] = acc

    def v_group(g):
        lhs = virt_v[g]
        for i in range(0, OCC, 2):
            parts = []
            for k in range(2):
                e = jnp.concatenate(
                    [e_all[pl.ds((src * 32 + g * QGRP) * OCC + i + k, QGRP, stride=OCC), :] for src in range(4)], 0)
                hi = e.astype(BF16)
                rest = e - hi.astype(F32)
                mid = rest.astype(BF16)
                low = (rest - mid.astype(F32)).astype(BF16)
                parts.append(jnp.concatenate([hi, mid, low], 0))
            v = dot(lhs, jnp.concatenate(parts, 1))
            for k in range(2):
                out_ref[i + k] += v[:, k * 128:k * 128 + LANES]

    def finish(g):
        y_own(g).wait_recv()
        q, n = OWN[g]
        rows = rows_of(q, n)
        e_all[rows_of(z * 32 + q, n)] = e_buf[y, z, rows] + y_in[z, rows]
        z_wait(n, zn_sem.at[g])
        for k in ((0, 1), (), (2,), (3,))[g]:
            z_wait(2 * CROSS_Q[k], zc_sem.at[k])
        if g == 1:
            unpack(0, 0, 15)
        if g == 2:
            unpack(1, 0, 9)
        if g == 3:
            unpack(1, 9, 15)
        v_group(g)

    def step(s, carry):
        @pl.when(s < STEPS)
        def _():
            a_wait(s)

            @pl.when(s + AHEAD < STEPS)
            def _():
                a_start(s + AHEAD)
            half_step(s)

            @pl.when(s == 0)
            def _():
                pl.semaphore_wait(barrier, 5)
            h_copy(s).start()

        def to_e(q, n, t):
            h_copy(t).wait_recv()
            e_step(q, n, t)
            y_cross(q, n, t).start()

        when_step(s, 0, STEPS, 1, to_e)

        for k in range(len(NEAR)):
            @pl.when(s == NEAR_AT[k])
            def _():
                y_near(k).start()

        for k in range(GROUPS):
            @pl.when(s == OWN_AT[k])
            def _():
                y_own(k).start()

        def to_z(q, n, t):
            y_cross(q, n, t).wait_recv()
            add_send(far, q, n, zc_sem.at[(q + n - 1) // QGRP])
            add_send(far_near, q, n, zc_sem.at[(q + n - 1) // QGRP])

        when_step(s, 0, SWITCH, CROSS_SUM, to_z)
        when_step(s, SWITCH, STEPS, CROSS_SUM_2, to_z)

        for k in range(len(NEAR)):
            @pl.when(s == NEAR_SUM[k])
            def _():
                y_near(k).wait_recv()
                add_send(near, *NEAR[k], zn_sem.at[NEAR[k][0] // QGRP])

        for g in range(GROUPS - 1):
            @pl.when(s == V_AT[g])
            def _():
                finish(g)
        return carry

    lax.fori_loop(0, END, step, 0)
    finish(GROUPS - 1)

    pltpu.make_async_remote_copy(
        src_ref=h_buf.at[1 - core], dst_ref=h_in, send_sem=hs_sem, recv_sem=hr_sem.at[0],
        device_id={"dev": sib}, device_id_type=MESH).wait_send()
    y_copy(0, 4, 0, KEPT, yo_sem.at[0]).wait_send()
    rows = pl.ds(0, 3 * KEPT * OCC)
    pltpu.make_async_remote_copy(
        src_ref=e_all.at[rows], dst_ref=e_all.at[rows], send_sem=zs_sem, recv_sem=zn_sem.at[0],
        device_id={"dev2": near}, device_id_type=MESH).wait_send()


def solution(mesh):
    def local_block(ao_blk, c_occ, c_virt):
        hbm = pl.BlockSpec(memory_space=pltpu.HBM)
        dma = pltpu.SemaphoreType.DMA
        return pl.pallas_call(
            kernel,
            out_shape=jax.ShapeDtypeStruct((OCC, VIRT, LANES), F32),
            in_specs=[hbm, hbm, hbm],
            out_specs=pl.BlockSpec(memory_space=pltpu.VMEM),
            scratch_shapes=[
                pltpu.VMEM((SLOTS, 32, 2, 128, 128), BF16),
                pltpu.VMEM((2 * OCC, 256), BF16),
                pltpu.VMEM((384, 256), BF16),
                pltpu.VMEM((192, 256), BF16),
                pltpu.VMEM((192, 256), BF16),
                pltpu.VMEM((GROUPS, VIRT, 96), BF16),
                pltpu.VMEM((2, 32, 256, 128), BF16),
                pltpu.VMEM((32, 256, 128), BF16),
                pltpu.VMEM((SPECIAL, 192, 128), F32),
                pltpu.VMEM((2, 4, PART, 128), F32),
                pltpu.VMEM((4, PART, 128), F32),
                pltpu.VMEM((4 * PART, 128), F32),
                pltpu.VMEM((OCC, 128), BF16),
                pltpu.VMEM((VIRT, 128), BF16),
                dma((2,)), dma((SLOTS,)),
                dma, dma((H_RING,)),
                dma, dma((Y_RING,)), dma((len(NEAR),)), dma((GROUPS,)),
                dma, dma((GROUPS,)), dma((GROUPS,)),
            ],
            compiler_params=pltpu.CompilerParams(
                collective_id=0, has_side_effects=True, vmem_limit_bytes=37 * 1024 * 1024),
        )(ao_blk, *(pltpu.with_memory_space_constraint(c.T, pltpu.HBM) for c in (c_occ, c_virt)))

    return jax.shard_map(
        local_block, mesh=mesh,
        in_specs=(P(("frag", "dev"), "dev2", None, None), P("frag", None), P("frag", None)),
        out_specs=P("frag", None, ("dev2", "dev")),
        check_vma=False)
```
